32 devices in a mesh: grp: 4 (over y, x), dev: 8 (over z, core).
Axes of the slice: x: 2, y: 2, z: 4, core: 2. Of those that a mesh axis runs over, the one named last changes fastest.
Arguments:
- table: bfloat16 [8, 32768, 256], P('grp', 'dev'), may hold values from -0.75 to 0.75
- token_ids: int32 [8192], P(('grp', 'dev')), may hold values from 0 to 32767, as said below
- hidden: bfloat16 [8192, 2560], P(('grp', 'dev')), may hold values from -6 to 6
- w_proj: bfloat16 [2560, 2048], replicated, may hold values from -0.125 to 0.125
- norm_gain: float32 [256], replicated, may hold values from 0.5 to 1.5
Outputs:
- served_table: bfloat16 [8, 4, 1024, 2048], P('dev', 'grp')
- layer_inputs: bfloat16 [8192, 8, 256], P(('grp', 'dev'))
The draws below stay inside these ranges and needn't reach their ends.
Inputs may be any that keep to these rules, and one draw needn't show every extreme that they name: `token_ids`: of the 256 tokens of one device, at most 16 have ids in any one aligned block of 1024 vocabulary rows, and exactly 16 in some block.
All inputs are finite; a program needn't handle non-finite values.
Results may differ from the reference program's by a relative error of at most 0.001.
Values may be sent and summed in bfloat16 or wider, within the bound.
A program may use at most 128 MiB of HBM per device.

```python
import math
import jax
import jax.numpy as jnp
from jax import lax

D = 2560
E = 256
LAYERS = 8
ROWS_DEV = 1024
TOK_DEV = 256
CAP = 16
VOCAB = 32768
TOKENS = 8192
N_GRP = 4
N_DEV = 8


def draw_token_ids(key, part):
    blocks = VOCAB // ROWS_DEV
    slots = blocks * CAP
    ranking = jax.random.permutation(jax.random.fold_in(key, 7), blocks).astype(jnp.int32)
    hotness = (ranking < max(blocks // 8, 1)).astype(jnp.int32)
    slot_ids = jnp.arange(slots, dtype=jnp.int32)
    slot_block = slot_ids // CAP

    def one_device(dev_key):
        key_full, key_score, key_order, key_first, key_second = jax.random.split(dev_key, 5)
        full_block = jax.random.randint(key_full, (), 0, blocks, dtype=jnp.int32)
        score = jax.random.randint(key_score, (slots,), 0, slots, dtype=jnp.int32) * slots + slot_ids
        score = score + jnp.take(hotness, slot_block) * slots * slots
        score = score + (slot_block == full_block).astype(jnp.int32) * 2 * slots * slots
        top_scores, chosen = lax.top_k(score, TOK_DEV)
        owners = (chosen.astype(jnp.int32) // CAP).astype(jnp.int32)
        order = jax.random.permutation(key_order, TOK_DEV)
        owners = owners[order]
        first = jax.random.randint(key_first, (TOK_DEV,), 0, ROWS_DEV, dtype=jnp.int32)
        second = jax.random.randint(key_second, (TOK_DEV,), 0, ROWS_DEV, dtype=jnp.int32)
        return owners * ROWS_DEV + jnp.minimum(first, second)
    dev_keys = jax.random.split(jax.random.fold_in(key, 11), blocks)
    return jax.vmap(one_device)(dev_keys).reshape(TOKENS).astype(jnp.int32)


def block_levels(stream_key, dims, pieces, low, top_value):
    loudness, own = 1.0, jax.random.fold_in(stream_key, 6)
    for position, parts in pieces:
        steps = jnp.exp(jax.random.uniform(jax.random.fold_in(own, position), (parts,), jnp.float32, low / len(pieces), top_value / len(pieces)))
        loudness = loudness * jnp.repeat(steps, dims[position] // parts).reshape([-1 if axis == position else 1 for axis in range(len(dims))])
    return loudness


def bell_draw(rng, extent, width, most, cuts=(), held_as=jnp.bfloat16):
    drawn = jax.random.normal(rng, extent, jnp.float32) * width
    if len(cuts) > 0:
        drawn = block_levels(rng, extent, cuts, -0.22, 0.18) * drawn
    return jnp.clip(drawn, min=-most, max=most).astype(held_as)


def setup_inputs(seed: int = 0) -> dict:
    seeds = jax.random.split(jax.random.key(seed), 6)
    table = bell_draw(seeds[0], (LAYERS, VOCAB, E), 0.125, 0.75, ((0, 4), (1, 8)))
    token_ids = draw_token_ids(jax.random.fold_in(seeds[5], 71), 0)
    hidden = bell_draw(seeds[2], (TOKENS, D), 1.0, 6.0, ((0, 32),))
    w_proj = bell_draw(seeds[3], (D, LAYERS * E), D ** -0.5, 0.125)
    norm_gain = jnp.clip(1.0 + 0.1 * jax.random.normal(seeds[4], (E,), jnp.float32), 0.5, 1.5)
    return dict(table=table, token_ids=token_ids, hidden=hidden, w_proj=w_proj, norm_gain=norm_gain)


def reference(table, token_ids, hidden, w_proj, norm_gain):
    served_table = jnp.transpose(table, (1, 0, 2)).reshape(N_DEV, N_GRP, ROWS_DEV, LAYERS * E)
    emb = jnp.transpose(jnp.take(table, token_ids, axis=1), (1, 0, 2)).astype(jnp.float32)
    proj = jnp.dot(hidden, w_proj, preferred_element_type=jnp.float32).reshape(TOKENS, LAYERS, E)
    mean_sq = lax.optimization_barrier(jnp.mean(proj * proj, axis=-1, keepdims=True))
    normed = proj / jnp.sqrt(mean_sq + 1e-06) * norm_gain
    layer_inputs = ((normed + math.sqrt(E) * emb) / math.sqrt(2.0)).astype(jnp.bfloat16)
    return (served_table, layer_inputs)
```

```python
import functools
import math

import jax
import jax.numpy as jnp
from jax import lax
from jax.experimental import pallas as pl
from jax.experimental.pallas import tpu as pltpu
from jax.sharding import PartitionSpec as P

MESH = pl.DeviceIdType.MESH
LANES = 128


def column(row):
    return jnp.transpose(jnp.broadcast_to(row.astype(jnp.float32), (LANES, LANES)))


def exchange(n_grp, n_dev, cap,
             ids_ref, want_ref, hidden_ref, gain_ref, table_ref, w_ref,
             served_ref, out_ref,
             tbl, wbuf, ids_buf, want_buf, cols, send, recv, esend, erecv, normed,
             ids_ss, ids_rs, want_ss, want_rs, tab_ss, tab_rs, z_ss, z_rs, e_ss, e_rs,
             tbl_sem, w_sem, own_sem):
    g = lax.axis_index("grp")
    d = lax.axis_index("dev")
    layer_share, vocab_share, width = table_ref.shape
    rows = vocab_share // n_grp
    tok = hidden_ref.shape[0]
    layers = layer_share * n_grp
    wide = layer_share * width
    slots = n_grp * cap
    all_slots = n_dev * slots

    def grp_at(i):
        return lax.rem(g + i, n_grp)

    def dev_at(j):
        return lax.rem(d + j, n_dev)

    load_table = pltpu.make_async_copy(table_ref, tbl, tbl_sem)
    load_table.start()
    load_w = pltpu.make_async_copy(w_ref, wbuf, w_sem)
    load_w.start()

    barrier = pltpu.get_barrier_semaphore()
    for i in range(n_grp):
        def greet(j, carry, i=i):
            pl.semaphore_signal(
                barrier, inc=1, device_id={"grp": grp_at(i), "dev": dev_at(j)}, device_id_type=MESH
            )
            return carry
        lax.fori_loop(1 if i == 0 else 0, n_dev, greet, 0)
    pl.semaphore_wait(barrier, n_grp * n_dev - 1)

    def ids_copy(i, j):
        return pltpu.make_async_remote_copy(
            src_ref=ids_ref.at[dev_at(j)], dst_ref=ids_buf.at[g, d],
            send_sem=ids_ss.at[i, j], recv_sem=ids_rs.at[i, j],
            device_id={"grp": grp_at(i), "dev": dev_at(j)}, device_id_type=MESH,
        )

    def want_copy(i):
        return pltpu.make_async_remote_copy(
            src_ref=want_ref, dst_ref=want_buf.at[g],
            send_sem=want_ss.at[i], recv_sem=want_rs.at[i],
            device_id={"grp": grp_at(i), "dev": d}, device_id_type=MESH,
        )

    order = list(range(n_grp - 1, 0, -1)) + [0]
    for i in [(n_grp - o) % n_grp for o in order]:
        def start_ids(j, carry, i=i):
            ids_copy(i, j).start()
            return carry
        lax.fori_loop(1 if i == 0 else 0, n_dev, start_ids, 0)
    for i in range(1, n_grp):
        want_copy(i).start()

    def tab_copy(i, l):
        gp = grp_at(i)
        return pltpu.make_async_remote_copy(
            src_ref=table_ref.at[l, pl.ds(pl.multiple_of(gp * rows, rows), rows), :],
            dst_ref=served_ref.at[:, pl.ds(pl.multiple_of((g * layer_share + l) * width, width), width)],
            send_sem=tab_ss.at[i, l], recv_sem=tab_rs.at[i, l],
            device_id={"grp": gp, "dev": d}, device_id_type=MESH,
        )

    for l in range(layer_share):
        for i in range(1, n_grp):
            tab_copy(i, l).start()

    def own_copy(l):
        return pltpu.make_async_copy(
            tbl.at[l, pl.ds(pl.multiple_of(g * rows, rows), rows), :],
            served_ref.at[:, pl.ds(pl.multiple_of((g * layer_share + l) * width, width), width)],
            own_sem.at[l],
        )

    load_table.wait()
    for l in range(layer_share):
        own_copy(l).start()

    ids_buf[g, d] = ids_ref[d]
    want_buf[g] = want_ref[...]

    def z_copy(o, j):
        dp = dev_at(j)
        gp = grp_at(o)
        return pltpu.make_async_remote_copy(
            src_ref=send.at[o, dp],
            dst_ref=recv.at[gp, pl.ds(pl.multiple_of(d * slots, slots), slots), :],
            send_sem=z_ss.at[o, j], recv_sem=z_rs.at[o, j],
            device_id={"grp": g, "dev": dp}, device_id_type=MESH,
        )

    for o in order:
        gp = grp_at(o)
        back = (n_grp - o) % n_grp

        def take_ids(j, carry, back=back):
            ids_copy(back, j).wait_recv()
            return carry
        lax.fori_loop(1 if back == 0 else 0, n_dev, take_ids, 0)

        def turn(a, carry, gp=gp):
            cols[a] = column(ids_buf[gp, a])
            return carry
        lax.fori_loop(0, n_dev, turn, 0)

        def block(b, carry, o=o):
            at = pl.multiple_of(b * cap, cap)
            wanted = cols[:, pl.ds(at, cap), :].reshape(n_dev * cap, LANES)
            lane = lax.broadcasted_iota(jnp.int32, (n_dev * cap, LANES), 1)
            lane = (lane + (d * n_grp + b) * rows).astype(jnp.float32)
            wanted = wanted - lane
            hit = jnp.concatenate(
                [(wanted == float(c * LANES)).astype(jnp.float32) for c in range(rows // LANES)], axis=1
            ).astype(jnp.bfloat16)
            for l in range(layer_share):
                found = jnp.dot(
                    hit, tbl[l, pl.ds(pl.multiple_of(b * rows, rows), rows), :],
                    preferred_element_type=jnp.float32,
                ).astype(jnp.bfloat16)
                send[o, :, pl.ds(at, cap), l * width:(l + 1) * width] = found.reshape(n_dev, cap, width)
            return carry
        lax.fori_loop(0, n_grp, block, 0)

        def start_z(j, carry, o=o):
            z_copy(o, j).start()
            return carry
        lax.fori_loop(1, n_dev, start_z, 0)
        recv[gp, pl.ds(pl.multiple_of(d * slots, slots), slots), :] = send[o, d]

    load_w.wait()

    def project(l, carry):
        at = pl.multiple_of(l * width, width)
        proj = jnp.dot(hidden_ref[...], wbuf[:, pl.ds(at, width)], preferred_element_type=jnp.float32)
        mean_sq = jnp.mean(proj * proj, axis=-1, keepdims=True)
        normed[l] = proj / jnp.sqrt(mean_sq + 1e-06) * gain_ref[...]
        return carry
    lax.fori_loop(0, layers, project, 0)

    def e_copy(o):
        return pltpu.make_async_remote_copy(
            src_ref=esend.at[o], dst_ref=erecv.at[g],
            send_sem=e_ss.at[o], recv_sem=e_rs.at[o],
            device_id={"grp": grp_at(o), "dev": d}, device_id_type=MESH,
        )

    for o in order:
        gp = grp_at(o)
        if o:
            want_copy(n_grp - o).wait_recv()

        def take_rows(j, carry, o=o):
            z_copy(o, j).wait_recv()
            return carry
        lax.fori_loop(1, n_dev, take_rows, 0)

        for t in range(tok // LANES):
            mine = column(want_buf[gp, t:t + 1, :])
            lane = lax.broadcasted_iota(jnp.int32, (LANES, LANES), 1).astype(jnp.float32)
            mine = mine - lane
            picker = jnp.concatenate(
                [(mine == float(c * LANES)).astype(jnp.float32) for c in range(all_slots // LANES)], axis=1
            ).astype(jnp.bfloat16)
            picked = jnp.dot(picker, recv[gp], preferred_element_type=jnp.float32).astype(jnp.bfloat16)
            if o:
                esend[o, t * LANES:(t + 1) * LANES, :] = picked
            else:
                erecv[g, t * LANES:(t + 1) * LANES, :] = picked
        if o:
            e_copy(o).start()

    for o in range(1, n_grp):
        e_copy(o).wait_recv()

    for l in range(layers):
        at = (l % layer_share) * width
        emb = erecv[l // layer_share, :, at:at + width].astype(jnp.float32)
        mixed = (normed[l] + math.sqrt(width) * emb) / math.sqrt(2.0)
        out_ref[:, l * width:(l + 1) * width] = mixed.astype(jnp.bfloat16)

    for l in range(layer_share):
        own_copy(l).wait()
        for i in range(1, n_grp):
            tab_copy(i, l).wait()
    for i in range(n_grp):
        def end_ids(j, carry, i=i):
            ids_copy(i, j).wait_send()
            return carry
        lax.fori_loop(1 if i == 0 else 0, n_dev, end_ids, 0)

        def end_z(j, carry, i=i):
            z_copy(i, j).wait_send()
            return carry
        lax.fori_loop(1, n_dev, end_z, 0)
        if i:
            want_copy(i).wait_send()
            e_copy(i).wait_send()


def on_device(table, token_ids, hidden, w_proj, norm_gain):
    n_grp = lax.axis_size("grp")
    n_dev = lax.axis_size("dev")
    layer_share, vocab_share, width = table.shape
    layers = layer_share * n_grp
    tok = token_ids.shape[0]
    rows = vocab_share // n_grp
    blocks = n_grp * n_dev
    cap = -(-max(2, 2 * tok // blocks) // 16) * 16
    slots = n_grp * cap
    assert slots <= LANES and tok % LANES == 0 and rows % LANES == 0
    wide = layer_share * width

    owner = token_ids // rows
    positions = jnp.arange(tok, dtype=jnp.int32)
    same = owner[:, None] == owner[None, :]
    earlier = positions[None, :] < positions[:, None]
    slot = jnp.sum((same & earlier).astype(jnp.int32), axis=1)
    wanted = owner * cap + slot
    hit = (wanted[:, None] == jnp.arange(blocks * cap, dtype=jnp.int32)[None, :]).astype(jnp.int32)
    outgoing = jnp.sum(hit * (token_ids + 1)[:, None], axis=0) - 1
    outgoing = outgoing.reshape(n_dev, 1, slots)
    outgoing = jnp.pad(outgoing, ((0, 0), (0, 0), (0, LANES - slots)), constant_values=-1)

    vmem = pl.BlockSpec(memory_space=pltpu.VMEM)
    anywhere = pl.BlockSpec(memory_space=pl.ANY)
    dma = pltpu.SemaphoreType.DMA
    bf16 = jnp.bfloat16
    served, mixed = pl.pallas_call(
        functools.partial(exchange, n_grp, n_dev, cap),
        out_shape=(
            jax.ShapeDtypeStruct((rows, layers * width), bf16),
            jax.ShapeDtypeStruct((tok, layers * width), bf16),
        ),
        in_specs=[vmem, vmem, vmem, vmem, anywhere, anywhere],
        out_specs=(anywhere, vmem),
        scratch_shapes=[
            pltpu.VMEM(table.shape, bf16),
            pltpu.VMEM(w_proj.shape, bf16),
            pltpu.VMEM((n_grp, n_dev, 1, LANES), jnp.int32),
            pltpu.VMEM((n_grp, tok // LANES, LANES), jnp.int32),
            pltpu.VMEM((n_dev, LANES, LANES), jnp.float32),
            pltpu.VMEM((n_grp, n_dev, slots, wide), bf16),
            pltpu.VMEM((n_grp, n_dev * slots, wide), bf16),
            pltpu.VMEM((n_grp, tok, wide), bf16),
            pltpu.VMEM((n_grp, tok, wide), bf16),
            pltpu.VMEM((layers, tok, width), jnp.float32),
            dma((n_grp, n_dev)), dma((n_grp, n_dev)),
            dma((n_grp,)), dma((n_grp,)),
            dma((n_grp, layer_share)), dma((n_grp, layer_share)),
            dma((n_grp, n_dev)), dma((n_grp, n_dev)),
            dma((n_grp,)), dma((n_grp,)),
            dma, dma, dma((layer_share,)),
        ],
        compiler_params=pltpu.CompilerParams(
            collective_id=0, has_side_effects=True, vmem_limit_bytes=56 * 2**20
        ),
        name="exchange",
    )(outgoing, wanted.reshape(tok // LANES, LANES), hidden, norm_gain.reshape(1, width), table, w_proj)
    return (
        served.reshape(1, 1, rows, layers * width),
        mixed.reshape(tok, layers, width),
    )


def solution(mesh):
    in_specs = (P("grp", "dev", None), P(("grp", "dev")), P(("grp", "dev"), None), P(), P())
    out_specs = (P("dev", "grp", None, None), P(("grp", "dev"), None, None))
    return jax.shard_map(
        on_device, mesh=mesh, in_specs=in_specs, out_specs=out_specs, check_vma=False
    )
```

```python
import functools
import math

import jax
import jax.numpy as jnp
from jax import lax
from jax.experimental import pallas as pl
from jax.experimental.pallas import tpu as pltpu
from jax.sharding import PartitionSpec as P

MESH = pl.DeviceIdType.MESH
LANES = 128
PIECES = 4


def column(row):
    return jnp.transpose(jnp.broadcast_to(row.astype(jnp.float32), (LANES, LANES)))


def exchange(n_grp, n_dev, cap,
             ids_ref, want_ref, hidden_ref, gain_ref, table_ref, w_ref,
             served_ref, out_ref,
             tbl, wbuf, ids_buf, want_buf, cols, send, recv, esend, erecv, mix,
             ids_ss, ids_rs, want_ss, want_rs, tab_ss, tab_rs, z_ss, z_rs, e_ss, e_rs,
             tbl_sem, w_sem, own_sem):
    g = lax.axis_index("grp")
    d = lax.axis_index("dev")
    layer_share, vocab_share, width = table_ref.shape
    rows = vocab_share // n_grp
    tok = hidden_ref.shape[0]
    layers = layer_share * n_grp
    wide = layer_share * width
    slots = n_grp * cap
    all_slots = n_dev * slots

    def grp_at(i):
        return lax.rem(g + i, n_grp)

    def dev_at(j):
        return lax.rem(d + j, n_dev)

    load_table = pltpu.make_async_copy(table_ref, tbl, tbl_sem)
    load_table.start()
    load_w = pltpu.make_async_copy(w_ref, wbuf, w_sem)
    load_w.start()

    barrier = pltpu.get_barrier_semaphore()
    for i in range(n_grp):
        def greet(j, carry, i=i):
            pl.semaphore_signal(
                barrier, inc=1, device_id={"grp": grp_at(i), "dev": dev_at(j)}, device_id_type=MESH
            )
            return carry
        lax.fori_loop(1 if i == 0 else 0, n_dev, greet, 0)
    pl.semaphore_wait(barrier, n_grp * n_dev - 1)

    def ids_copy(i, j):
        return pltpu.make_async_remote_copy(
            src_ref=ids_ref.at[dev_at(j)], dst_ref=ids_buf.at[g, d],
            send_sem=ids_ss.at[i, j], recv_sem=ids_rs.at[i, j],
            device_id={"grp": grp_at(i), "dev": dev_at(j)}, device_id_type=MESH,
        )

    def want_copy(i):
        return pltpu.make_async_remote_copy(
            src_ref=want_ref, dst_ref=want_buf.at[g],
            send_sem=want_ss.at[i], recv_sem=want_rs.at[i],
            device_id={"grp": grp_at(i), "dev": d}, device_id_type=MESH,
        )

    order = list(range(n_grp - 1, 0, -1)) + [0]
    for i in [(n_grp - o) % n_grp for o in order]:
        def start_ids(j, carry, i=i):
            ids_copy(i, j).start()
            return carry
        lax.fori_loop(1 if i == 0 else 0, n_dev, start_ids, 0)
    for i in range(1, n_grp):
        want_copy(i).start()

    part = rows // PIECES
    pieces = [(l, p) for l in range(layer_share) for p in range(PIECES)]

    def tab_copy(i, l, p):
        gp = grp_at(i)
        return pltpu.make_async_remote_copy(
            src_ref=table_ref.at[l, pl.ds(pl.multiple_of(gp * rows + p * part, part), part), :],
            dst_ref=served_ref.at[
                pl.ds(p * part, part),
                pl.ds(pl.multiple_of((g * layer_share + l) * width, width), width),
            ],
            send_sem=tab_ss.at[i, l, p], recv_sem=tab_rs.at[i, l, p],
            device_id={"grp": gp, "dev": d}, device_id_type=MESH,
        )

    def start_pieces(first, last):
        for l, p in pieces[first:last]:
            for i in range(1, n_grp):
                tab_copy(i, l, p).start()

    ahead = len(pieces) * 3 // 4
    middle = len(pieces) * 7 // 8
    start_pieces(0, ahead)

    def own_copy(l):
        return pltpu.make_async_copy(
            table_ref.at[l, pl.ds(pl.multiple_of(g * rows, rows), rows), :],
            served_ref.at[:, pl.ds(pl.multiple_of((g * layer_share + l) * width, width), width)],
            own_sem.at[l],
        )

    for l in range(layer_share):
        own_copy(l).start()
    load_table.wait()

    ids_buf[g, d] = ids_ref[d]
    want_buf[g] = want_ref[...]

    def z_copy(o, j):
        dp = dev_at(j)
        gp = grp_at(o)
        return pltpu.make_async_remote_copy(
            src_ref=send.at[o, dp],
            dst_ref=recv.at[gp, pl.ds(pl.multiple_of(d * slots, slots), slots), :],
            send_sem=z_ss.at[o, j], recv_sem=z_rs.at[o, j],
            device_id={"grp": g, "dev": dp}, device_id_type=MESH,
        )

    for o in order:
        gp = grp_at(o)
        back = (n_grp - o) % n_grp

        def take_ids(j, carry, back=back):
            ids_copy(back, j).wait_recv()
            return carry
        lax.fori_loop(1 if back == 0 else 0, n_dev, take_ids, 0)

        def turn(a, carry, gp=gp):
            cols[a] = column(ids_buf[gp, a])
            return carry
        lax.fori_loop(0, n_dev, turn, 0)

        def block(b, carry, o=o):
            at = pl.multiple_of(b * cap, cap)
            wanted = cols[:, pl.ds(at, cap), :].reshape(n_dev * cap, LANES)
            lane = lax.broadcasted_iota(jnp.int32, (n_dev * cap, LANES), 1)
            lane = (lane + (d * n_grp + b) * rows).astype(jnp.float32)
            wanted = wanted - lane
            hit = jnp.concatenate(
                [(wanted == float(c * LANES)).astype(jnp.float32) for c in range(rows // LANES)], axis=1
            ).astype(jnp.bfloat16)
            for l in range(layer_share):
                found = jnp.dot(
                    hit, tbl[l, pl.ds(pl.multiple_of(b * rows, rows), rows), :],
                    preferred_element_type=jnp.float32,
                ).astype(jnp.bfloat16)
                send[o, :, pl.ds(at, cap), l * width:(l + 1) * width] = found.reshape(n_dev, cap, width)
            return carry
        lax.fori_loop(0, n_grp, block, 0)

        def start_z(j, carry, o=o):
            z_copy(o, j).start()
            return carry
        lax.fori_loop(1, n_dev, start_z, 0)
        recv[gp, pl.ds(pl.multiple_of(d * slots, slots), slots), :] = send[o, d]

    load_w.wait()

    def project(l):
        proj = jnp.dot(hidden_ref[...], wbuf[:, l * width:(l + 1) * width], preferred_element_type=jnp.float32)
        mean_sq = jnp.mean(proj * proj, axis=-1, keepdims=True)
        return proj / jnp.sqrt(mean_sq + 1e-06) * gain_ref[...]

    for l in range(layers):
        mix[:, l, :] = project(l)

    def e_copy(o):
        return pltpu.make_async_remote_copy(
            src_ref=esend.at[o], dst_ref=erecv.at[g],
            send_sem=e_ss.at[o], recv_sem=e_rs.at[o],
            device_id={"grp": grp_at(o), "dev": d}, device_id_type=MESH,
        )

    for o in order:
        gp = grp_at(o)
        if o:
            want_copy(n_grp - o).wait_recv()

        def take_rows(j, carry, o=o):
            z_copy(o, j).wait_recv()
            return carry
        lax.fori_loop(1, n_dev, take_rows, 0)

        for t in range(tok // LANES):
            mine = column(want_buf[gp, t:t + 1, :])
            lane = lax.broadcasted_iota(jnp.int32, (LANES, LANES), 1).astype(jnp.float32)
            mine = mine - lane
            picker = jnp.concatenate(
                [(mine == float(c * LANES)).astype(jnp.float32) for c in range(all_slots // LANES)], axis=1
            ).astype(jnp.bfloat16)
            picked = jnp.dot(picker, recv[gp], preferred_element_type=jnp.float32).astype(jnp.bfloat16)
            if o:
                esend[o, t * LANES:(t + 1) * LANES, :] = picked
            else:
                erecv[g, t * LANES:(t + 1) * LANES, :] = picked
        if o:
            e_copy(o).start()
        if o == order[-3 if n_grp > 2 else -2]:
            start_pieces(ahead, middle)
        if o == order[-2]:
            start_pieces(middle, len(pieces))

    for o in range(1, n_grp):
        e_copy(o).wait_recv()

    for l in range(layers):
        at = (l % layer_share) * width
        emb = erecv[l // layer_share, :, at:at + width].astype(jnp.float32)
        mix[:, l, :] = (mix[:, l, :] + math.sqrt(width) * emb) / math.sqrt(2.0)
    out_ref[...] = mix[...].astype(jnp.bfloat16)

    for l in range(layer_share):
        own_copy(l).wait()
    for l, p in pieces:
        for i in range(1, n_grp):
            tab_copy(i, l, p).wait()
    for i in range(n_grp):
        def end_ids(j, carry, i=i):
            ids_copy(i, j).wait_send()
            return carry
        lax.fori_loop(1 if i == 0 else 0, n_dev, end_ids, 0)

        def end_z(j, carry, i=i):
            z_copy(i, j).wait_send()
            return carry
        lax.fori_loop(1, n_dev, end_z, 0)
        if i:
            want_copy(i).wait_send()
            e_copy(i).wait_send()


def on_device(table, token_ids, hidden, w_proj, norm_gain):
    n_grp = lax.axis_size("grp")
    n_dev = lax.axis_size("dev")
    layer_share, vocab_share, width = table.shape
    layers = layer_share * n_grp
    tok = token_ids.shape[0]
    rows = vocab_share // n_grp
    blocks = n_grp * n_dev
    cap = -(-max(2, 2 * tok // blocks) // 16) * 16
    slots = n_grp * cap
    assert slots <= LANES and tok % LANES == 0 and rows % LANES == 0
    wide = layer_share * width

    owner = token_ids // rows
    positions = jnp.arange(tok, dtype=jnp.int32)
    same = owner[:, None] == owner[None, :]
    earlier = positions[None, :] < positions[:, None]
    slot = jnp.sum((same & earlier).astype(jnp.int32), axis=1)
    wanted = owner * cap + slot
    hit = (wanted[:, None] == jnp.arange(blocks * cap, dtype=jnp.int32)[None, :]).astype(jnp.int32)
    outgoing = jnp.sum(hit * (token_ids + 1)[:, None], axis=0) - 1
    outgoing = outgoing.reshape(n_dev, 1, slots)
    outgoing = jnp.pad(outgoing, ((0, 0), (0, 0), (0, LANES - slots)), constant_values=-1)

    vmem = pl.BlockSpec(memory_space=pltpu.VMEM)
    anywhere = pl.BlockSpec(memory_space=pl.ANY)
    dma = pltpu.SemaphoreType.DMA
    bf16 = jnp.bfloat16
    served, mixed = pl.pallas_call(
        functools.partial(exchange, n_grp, n_dev, cap),
        out_shape=(
            pltpu.VMEM((rows, layers * width), bf16),
            pltpu.VMEM((tok, layers, width), bf16),
        ),
        in_specs=[vmem, vmem, vmem, vmem, anywhere, anywhere],
        out_specs=(vmem, vmem),
        scratch_shapes=[
            pltpu.VMEM(table.shape, bf16),
            pltpu.VMEM(w_proj.shape, bf16),
            pltpu.VMEM((n_grp, n_dev, 1, LANES), jnp.int32),
            pltpu.VMEM((n_grp, tok // LANES, LANES), jnp.int32),
            pltpu.VMEM((n_dev, LANES, LANES), jnp.float32),
            pltpu.VMEM((n_grp, n_dev, slots, wide), bf16),
            pltpu.VMEM((n_grp, n_dev * slots, wide), bf16),
            pltpu.VMEM((n_grp, tok, wide), bf16),
            pltpu.VMEM((n_grp, tok, wide), bf16),
            pltpu.VMEM((tok, layers, width), jnp.float32),
            dma((n_grp, n_dev)), dma((n_grp, n_dev)),
            dma((n_grp,)), dma((n_grp,)),
            dma((n_grp, layer_share, PIECES)), dma((n_grp, layer_share, PIECES)),
            dma((n_grp, n_dev)), dma((n_grp, n_dev)),
            dma((n_grp,)), dma((n_grp,)),
            dma, dma, dma((layer_share,)),
        ],
        compiler_params=pltpu.CompilerParams(
            collective_id=0, has_side_effects=True, vmem_limit_bytes=44 * 2**20
        ),
        name="exchange",
    )(outgoing, wanted.reshape(tok // LANES, LANES), hidden, norm_gain.reshape(1, width), table, w_proj)
    return (served.reshape(1, 1, rows, layers * width), mixed)


def solution(mesh):
    in_specs = (P("grp", "dev", None), P(("grp", "dev")), P(("grp", "dev"), None), P(), P())
    out_specs = (P("dev", "grp", None, None), P(("grp", "dev"), None, None))
    return jax.shard_map(
        on_device, mesh=mesh, in_specs=in_specs, out_specs=out_specs, check_vma=False
    )
```

```python
import functools
import math

import jax
import jax.numpy as jnp
from jax import lax
from jax.experimental import pallas as pl
from jax.experimental.pallas import tpu as pltpu
from jax.sharding import PartitionSpec as P

MESH = pl.DeviceIdType.MESH
LANES = 128
PIECES = 4


def column(row):
    return jnp.transpose(jnp.broadcast_to(row.astype(jnp.float32), (LANES, LANES)))


def exchange(n_grp, n_dev, cap,
             ids_ref, want_ref, hidden_hbm, gain_hbm, table_ref, w_ref,
             served_ref, out_ref,
             hidden_ref, gain_ref, tbl, wbuf, ids_buf, want_buf, cols, send, recv, esend, erecv, mix,
             ids_ss, ids_rs, want_ss, want_rs, tab_ss, tab_rs, z_ss, z_rs, e_ss, e_rs,
             tbl_sem, w_sem, hidden_sem, gain_sem, own_sem):
    g = lax.axis_index("grp")
    d = lax.axis_index("dev")
    layer_share, vocab_share, width = table_ref.shape
    rows = vocab_share // n_grp
    tok = hidden_ref.shape[0]
    layers = layer_share * n_grp
    wide = layer_share * width
    slots = n_grp * cap
    all_slots = n_dev * slots

    def grp_at(i):
        return lax.rem(g + i, n_grp)

    def dev_at(j):
        return lax.rem(d + j, n_dev)

    load_table = pltpu.make_async_copy(table_ref, tbl, tbl_sem)
    load_table.start()
    load_w = pltpu.make_async_copy(w_ref, wbuf, w_sem)
    load_w.start()
    load_hidden = pltpu.make_async_copy(hidden_hbm, hidden_ref, hidden_sem)
    load_hidden.start()
    load_gain = pltpu.make_async_copy(gain_hbm, gain_ref, gain_sem)
    load_gain.start()

    barrier = pltpu.get_barrier_semaphore()
    for i in range(n_grp):
        def greet(j, carry, i=i):
            pl.semaphore_signal(
                barrier, inc=1, device_id={"grp": grp_at(i), "dev": dev_at(j)}, device_id_type=MESH
            )
            return carry
        lax.fori_loop(1 if i == 0 else 0, n_dev, greet, 0)
    pl.semaphore_wait(barrier, n_grp * n_dev - 1)

    def ids_copy(i, j):
        return pltpu.make_async_remote_copy(
            src_ref=ids_ref.at[dev_at(j)], dst_ref=ids_buf.at[g, d],
            send_sem=ids_ss.at[i, j], recv_sem=ids_rs.at[i, j],
            device_id={"grp": grp_at(i), "dev": dev_at(j)}, device_id_type=MESH,
        )

    def want_copy(i):
        return pltpu.make_async_remote_copy(
            src_ref=want_ref, dst_ref=want_buf.at[g],
            send_sem=want_ss.at[i], recv_sem=want_rs.at[i],
            device_id={"grp": grp_at(i), "dev": d}, device_id_type=MESH,
        )

    order = list(range(n_grp - 1, 0, -1)) + [0]
    for i in [(n_grp - o) % n_grp for o in order]:
        def start_ids(j, carry, i=i):
            ids_copy(i, j).start()
            return carry
        lax.fori_loop(1 if i == 0 else 0, n_dev, start_ids, 0)
    for i in range(1, n_grp):
        want_copy(i).start()

    part = rows // PIECES
    pieces = [(l, p) for l in range(layer_share) for p in range(PIECES)]

    def tab_copy(i, l, p):
        gp = grp_at(i)
        return pltpu.make_async_remote_copy(
            src_ref=table_ref.at[l, pl.ds(pl.multiple_of(gp * rows + p * part, part), part), :],
            dst_ref=served_ref.at[
                pl.ds(p * part, part),
                pl.ds(pl.multiple_of((g * layer_share + l) * width, width), width),
            ],
            send_sem=tab_ss.at[i, l, p], recv_sem=tab_rs.at[i, l, p],
            device_id={"grp": gp, "dev": d}, device_id_type=MESH,
        )

    def start_pieces(first, last):
        for l, p in pieces[first:last]:
            for i in range(1, n_grp):
                tab_copy(i, l, p).start()

    ahead = len(pieces) * 7 // 8
    start_pieces(0, ahead)

    def own_copy(l):
        return pltpu.make_async_copy(
            table_ref.at[l, pl.ds(pl.multiple_of(g * rows, rows), rows), :],
            served_ref.at[:, pl.ds(pl.multiple_of((g * layer_share + l) * width, width), width)],
            own_sem.at[l],
        )

    for l in range(layer_share):
        own_copy(l).start()
    load_table.wait()

    ids_buf[g, d] = ids_ref[d]
    want_buf[g] = want_ref[...]

    def z_copy(o, j):
        dp = dev_at(j)
        gp = grp_at(o)
        return pltpu.make_async_remote_copy(
            src_ref=send.at[o, dp],
            dst_ref=recv.at[gp, pl.ds(pl.multiple_of(d * slots, slots), slots), :],
            send_sem=z_ss.at[o, j], recv_sem=z_rs.at[o, j],
            device_id={"grp": g, "dev": dp}, device_id_type=MESH,
        )

    for o in order:
        gp = grp_at(o)
        back = (n_grp - o) % n_grp

        def take_ids(j, carry, back=back):
            ids_copy(back, j).wait_recv()
            return carry
        lax.fori_loop(1 if back == 0 else 0, n_dev, take_ids, 0)

        def turn(a, carry, gp=gp):
            cols[a] = column(ids_buf[gp, a])
            return carry
        lax.fori_loop(0, n_dev, turn, 0)

        def block(b, carry, o=o):
            at = pl.multiple_of(b * cap, cap)
            wanted = cols[:, pl.ds(at, cap), :].reshape(n_dev * cap, LANES)
            lane = lax.broadcasted_iota(jnp.int32, (n_dev * cap, LANES), 1)
            lane = (lane + (d * n_grp + b) * rows).astype(jnp.float32)
            wanted = wanted - lane
            hit = jnp.concatenate(
                [(wanted == float(c * LANES)).astype(jnp.float32) for c in range(rows // LANES)], axis=1
            ).astype(jnp.bfloat16)
            for l in range(layer_share):
                found = jnp.dot(
                    hit, tbl[l, pl.ds(pl.multiple_of(b * rows, rows), rows), :],
                    preferred_element_type=jnp.float32,
                ).astype(jnp.bfloat16)
                send[o, :, pl.ds(at, cap), l * width:(l + 1) * width] = found.reshape(n_dev, cap, width)
            return carry
        lax.fori_loop(0, n_grp, block, 0)

        def start_z(j, carry, o=o):
            z_copy(o, j).start()
            return carry
        lax.fori_loop(1, n_dev, start_z, 0)
        recv[gp, pl.ds(pl.multiple_of(d * slots, slots), slots), :] = send[o, d]

    load_w.wait()
    load_hidden.wait()
    load_gain.wait()

    def project(l):
        proj = jnp.dot(hidden_ref[...], wbuf[:, l * width:(l + 1) * width], preferred_element_type=jnp.float32)
        mean_sq = jnp.mean(proj * proj, axis=-1, keepdims=True)
        return proj / jnp.sqrt(mean_sq + 1e-06) * gain_ref[...]

    for l in range(layers):
        mix[:, l, :] = project(l)

    def e_copy(o):
        return pltpu.make_async_remote_copy(
            src_ref=esend.at[o], dst_ref=erecv.at[g],
            send_sem=e_ss.at[o], recv_sem=e_rs.at[o],
            device_id={"grp": grp_at(o), "dev": d}, device_id_type=MESH,
        )

    for o in order:
        gp = grp_at(o)
        if o:
            want_copy(n_grp - o).wait_recv()

        def take_rows(j, carry, o=o):
            z_copy(o, j).wait_recv()
            return carry
        lax.fori_loop(1, n_dev, take_rows, 0)

        for t in range(tok // LANES):
            mine = column(want_buf[gp, t:t + 1, :])
            lane = lax.broadcasted_iota(jnp.int32, (LANES, LANES), 1).astype(jnp.float32)
            mine = mine - lane
            picker = jnp.concatenate(
                [(mine == float(c * LANES)).astype(jnp.float32) for c in range(all_slots // LANES)], axis=1
            ).astype(jnp.bfloat16)
            picked = jnp.dot(picker, recv[gp], preferred_element_type=jnp.float32).astype(jnp.bfloat16)
            if o:
                esend[o, t * LANES:(t + 1) * LANES, :] = picked
            else:
                erecv[g, t * LANES:(t + 1) * LANES, :] = picked
        if o:
            e_copy(o).start()
        if o == order[-2]:
            start_pieces(ahead, len(pieces))

    for o in range(1, n_grp):
        e_copy(o).wait_recv()

    for l in range(layers):
        at = (l % layer_share) * width
        emb = erecv[l // layer_share, :, at:at + width].astype(jnp.float32)
        mix[:, l, :] = (mix[:, l, :] + math.sqrt(width) * emb) / math.sqrt(2.0)
    out_ref[...] = mix[...].astype(jnp.bfloat16)

    for l in range(layer_share):
        own_copy(l).wait()
    for l, p in pieces:
        for i in range(1, n_grp):
            tab_copy(i, l, p).wait()
    for i in range(n_grp):
        def end_ids(j, carry, i=i):
            ids_copy(i, j).wait_send()
            return carry
        lax.fori_loop(1 if i == 0 else 0, n_dev, end_ids, 0)

        def end_z(j, carry, i=i):
            z_copy(i, j).wait_send()
            return carry
        lax.fori_loop(1, n_dev, end_z, 0)
        if i:
            want_copy(i).wait_send()
            e_copy(i).wait_send()


def on_device(table, token_ids, hidden, w_proj, norm_gain):
    n_grp = lax.axis_size("grp")
    n_dev = lax.axis_size("dev")
    layer_share, vocab_share, width = table.shape
    layers = layer_share * n_grp
    tok = token_ids.shape[0]
    rows = vocab_share // n_grp
    blocks = n_grp * n_dev
    cap = -(-max(2, 2 * tok // blocks) // 16) * 16
    slots = n_grp * cap
    assert slots <= LANES and tok % LANES == 0 and rows % LANES == 0
    wide = layer_share * width

    owner = token_ids // rows
    positions = jnp.arange(tok, dtype=jnp.int32)
    same = owner[:, None] == owner[None, :]
    earlier = positions[None, :] < positions[:, None]
    slot = jnp.sum((same & earlier).astype(jnp.int32), axis=1)
    wanted = owner * cap + slot
    hit = (wanted[:, None] == jnp.arange(blocks * cap, dtype=jnp.int32)[None, :]).astype(jnp.int32)
    outgoing = jnp.sum(hit * (token_ids + 1)[:, None], axis=0) - 1
    outgoing = outgoing.reshape(n_dev, 1, slots)
    outgoing = jnp.pad(outgoing, ((0, 0), (0, 0), (0, LANES - slots)), constant_values=-1)

    vmem = pl.BlockSpec(memory_space=pltpu.VMEM)
    hbm = pl.BlockSpec(memory_space=pltpu.HBM)
    dma = pltpu.SemaphoreType.DMA
    bf16 = jnp.bfloat16
    served, mixed = pl.pallas_call(
        functools.partial(exchange, n_grp, n_dev, cap),
        out_shape=(
            pltpu.VMEM((rows, layers * width), bf16),
            pltpu.VMEM((tok, layers, width), bf16),
        ),
        in_specs=[vmem, vmem, hbm, hbm, hbm, hbm],
        out_specs=(vmem, vmem),
        scratch_shapes=[
            pltpu.VMEM(hidden.shape, bf16),
            pltpu.VMEM((1, width), jnp.float32),
            pltpu.VMEM(table.shape, bf16),
            pltpu.VMEM(w_proj.shape, bf16),
            pltpu.VMEM((n_grp, n_dev, 1, LANES), jnp.int32),
            pltpu.VMEM((n_grp, tok // LANES, LANES), jnp.int32),
            pltpu.VMEM((n_dev, LANES, LANES), jnp.float32),
            pltpu.VMEM((n_grp, n_dev, slots, wide), bf16),
            pltpu.VMEM((n_grp, n_dev * slots, wide), bf16),
            pltpu.VMEM((n_grp, tok, wide), bf16),
            pltpu.VMEM((n_grp, tok, wide), bf16),
            pltpu.VMEM((tok, layers, width), jnp.float32),
            dma((n_grp, n_dev)), dma((n_grp, n_dev)),
            dma((n_grp,)), dma((n_grp,)),
            dma((n_grp, layer_share, PIECES)), dma((n_grp, layer_share, PIECES)),
            dma((n_grp, n_dev)), dma((n_grp, n_dev)),
            dma((n_grp,)), dma((n_grp,)),
            dma, dma, dma, dma, dma((layer_share,)),
        ],
        compiler_params=pltpu.CompilerParams(
            collective_id=0, has_side_effects=True, vmem_limit_bytes=44 * 2**20
        ),
        name="exchange",
    )(outgoing, wanted.reshape(tok // LANES, LANES), hidden, norm_gain.reshape(1, width), table, w_proj)
    return (served.reshape(1, 1, rows, layers * width), mixed)


def solution(mesh):
    in_specs = (P("grp", "dev", None), P(("grp", "dev")), P(("grp", "dev"), None), P(), P())
    out_specs = (P("dev", "grp", None, None), P(("grp", "dev"), None, None))
    return jax.shard_map(
        on_device, mesh=mesh, in_specs=in_specs, out_specs=out_specs, check_vma=False
    )
```
